32 devices in a mesh: cell: 8 (over z, x), gene: 4 (over y, core).
Axes of the slice: x: 2, y: 2, z: 4, core: 2. Of those that a mesh axis runs over, the one named last changes fastest.
Arguments:
- counts: int32 [2048, 4096], P('cell', 'gene'), may hold values from 0 to 7
- totals: int32 [2048], P('cell'), may hold values from 1000 to 19999
- cell_factors: float32 [2048, 32], P('cell'), may hold values from -0.9 to 0.9
- gene_loadings: float32 [4096, 32], P('gene'), may hold values from -0.9 to 0.9
Outputs:
- new_factors: float32 [2048, 32], P('cell')
- new_loadings: float32 [4096, 32], P('gene')
- deviance: float32 [4096], P('gene')
The draws below stay inside these ranges and needn't reach their ends.
All inputs are finite; a program needn't handle non-finite values.
Results may differ from the reference program's by a relative error of at most 0.0044.
Values sent between devices are 32-bit elements; how exact they have to be, the bound alone decides.
No kernel may reach another device: no remote copies, remote signals or barrier semaphores. Data moves between devices by JAX's collectives and lax.ppermute only.
A program may use at most 128 MiB of HBM per device.

```python
import math
import jax
import jax.numpy as jnp
from jax import lax

L = 32
GENES = 4096
CD = 256
CELLS = 2048
N_CELL = 8


def set_ends(result, rng, smallest, largest):
    shape = result.shape
    place = [jax.random.randint(jax.random.fold_in(rng, axis), (), 0, shape[axis]) for axis in range(len(shape))]
    result = result.at[tuple(place)].set(smallest)
    longest = shape.index(max(shape))
    place[longest] = (place[longest] + 1) % shape[longest]
    return result.at[tuple(place)].set(largest)


def block_levels(stream_key, shape, shards, smallest, top_value):
    gain = 1.0
    for dim, parts in shards:
        draws = jax.random.uniform(jax.random.fold_in(jax.random.fold_in(stream_key, 6), dim), (parts,), jnp.float32, smallest / len(shards), top_value / len(shards))
        gain = gain * jnp.repeat(jnp.exp(draws), shape[dim] // parts).reshape((-1,) + (1,) * (len(shape) - 1 - dim))
    return gain


def gaussian(rng, extent, deviation, bound, shards=(), dtype=jnp.bfloat16):
    result = deviation * jax.random.normal(rng, extent, jnp.float32)
    if shards:
        result = result * block_levels(rng, extent, shards, -0.22, 0.18)
    return jnp.clip(result, -bound, bound).astype(dtype)


def setup_inputs(seed: int = 0) -> dict:
    keys = jax.random.split(jax.random.key(seed), 5)
    counts = set_ends(jax.random.randint(keys[0], (CELLS, GENES), 0, 8), jax.random.fold_in(keys[0], 1), 0, 7).astype(jnp.int32)
    totals = set_ends(jax.random.randint(keys[1], (CELLS,), 1000, 20000), jax.random.fold_in(keys[1], 1), 1000, 19999).astype(jnp.int32)
    cell_factors = gaussian(keys[2], (CELLS, L), 0.15, 0.9, ((0, 8),), jnp.float32)
    gene_loadings = gaussian(keys[3], (GENES, L), 0.15, 0.9, ((0, 4),), jnp.float32)
    return {"counts": counts, "totals": totals, "cell_factors": cell_factors, "gene_loadings": gene_loadings}


RIDGE = 1.0
DAMPING = 0.1
SCALE_TOTAL = 5000.0

def outer_table(factors):
    width = factors.shape[1]
    product = factors[:, :, None] * factors[:, None, :]
    return product.reshape(factors.shape[0], width * width).astype(jnp.bfloat16)

def newton_solve(curvature, gradient):
    width = gradient.shape[1]
    matrix = jnp.transpose(curvature.reshape(gradient.shape[0], width, width), (1, 2, 0))
    diagonal_mean = sum((matrix[index, index] for index in range(width))) / width
    shift = RIDGE + DAMPING * diagonal_mean
    right = jnp.transpose(gradient)
    columns = []
    for column in range(width):
        current = matrix[:, column]
        if column > 0:
            stacked = jnp.stack(columns)
            current = current - lax.optimization_barrier(jnp.sum(stacked * stacked[:, column][:, None, :], axis=0))
        current = current + jnp.where(jnp.arange(width) == column, 1.0, 0.0).astype(jnp.float32)[:, None] * shift[None, :]
        pivot = jnp.sqrt(current[column])
        mask = (jnp.arange(width) >= column).astype(jnp.float32)[:, None]
        columns.append(mask * current / pivot[None, :])
    lower = jnp.stack(columns, axis=1)
    forward = []
    for row in range(width):
        value = right[row]
        for inner in range(row):
            value = value - lower[row, inner] * forward[inner]
        forward.append(value / lower[row, row])
    backward = [None] * width
    for row in range(width - 1, -1, -1):
        value = forward[row]
        for inner in range(row + 1, width):
            value = value - lower[inner, row] * backward[inner]
        backward[row] = value / lower[row, row]
    return jnp.transpose(jnp.stack(backward))

def predict(offset, factors, loadings):
    linear = offset[:, None] + jnp.dot(factors, loadings.T, precision=lax.Precision.HIGHEST)
    return (linear, jnp.exp(linear))

def gene_contract(counts, expected, loadings):
    weights = expected.astype(jnp.bfloat16)
    residual = (counts.astype(jnp.float32) - expected).astype(jnp.bfloat16)
    gradient = jnp.dot(residual, loadings.astype(jnp.bfloat16), preferred_element_type=jnp.float32)
    curvature = jnp.dot(weights, outer_table(loadings), preferred_element_type=jnp.float32)
    return (gradient, curvature)

def cell_contract(counts, linear, expected, factors):
    counts_real = counts.astype(jnp.float32)
    weights = expected.astype(jnp.bfloat16)
    residual = (counts_real - expected).astype(jnp.bfloat16)
    dims = (((0,), (0,)), ((), ()))
    gradient = lax.dot_general(residual, factors.astype(jnp.bfloat16), dims, preferred_element_type=jnp.float32)
    curvature = lax.dot_general(weights, outer_table(factors), dims, preferred_element_type=jnp.float32)
    terms = 2.0 * (counts_real * (jnp.log(jnp.maximum(counts_real, 1.0)) - linear) - counts_real + expected)
    return (gradient, curvature, lax.optimization_barrier(jnp.sum(terms, axis=0)))

def reference(counts, totals, cell_factors, gene_loadings):
    offset = jnp.log(totals.astype(jnp.float32)) - math.log(SCALE_TOTAL)
    count_blocks = counts.reshape(N_CELL, CD, GENES)
    offset_blocks = offset.reshape(N_CELL, CD)
    factor_blocks = cell_factors.reshape(N_CELL, CD, L)

    def factor_update(block):
        count_block, offset_block, factor_block = block
        linear, expected = predict(offset_block, factor_block, gene_loadings)
        gradient, curvature = gene_contract(count_block, expected, gene_loadings)
        return factor_block + newton_solve(curvature, gradient - RIDGE * factor_block)
    new_blocks = lax.map(factor_update, (count_blocks, offset_blocks, factor_blocks))
    new_factors = new_blocks.reshape(CELLS, L)

    def loading_update(running, block):
        count_block, offset_block, factor_block = block
        linear, expected = predict(offset_block, factor_block, gene_loadings)
        gradient, curvature, deviance_part = cell_contract(count_block, linear, expected, factor_block)
        return ((running[0] + gradient, running[1] + curvature, running[2] + deviance_part), None)
    initial = (jnp.zeros((GENES, L), jnp.float32), jnp.zeros((GENES, L * L), jnp.float32), jnp.zeros((GENES,), jnp.float32))
    totals_sum, unused = lax.scan(loading_update, initial, (count_blocks, offset_blocks, new_blocks))
    gradient_sum, curvature_sum, deviance_sum = totals_sum
    new_loadings = gene_loadings + newton_solve(curvature_sum, gradient_sum - RIDGE * gene_loadings)
    deviance = deviance_sum / CELLS
    return (new_factors, new_loadings, deviance)
```

```python
import functools
import math

import jax
import jax.numpy as jnp
from jax import lax
from jax.experimental import pallas as pl
from jax.experimental.pallas import tpu as pltpu
from jax.sharding import PartitionSpec as P

RIDGE = 1.0
DAMPING = 0.1
SCALE_TOTAL = 5000.0
SUB = 8
LANES = 128
VMEM_LIMIT = 60 * 1024 * 1024


def table_pieces(width):
    return [(a, q) for a in range(width) for q in range(a // SUB, width // SUB)]


def fill_table(table_ref, x, width):
    pieces = table_pieces(width)
    chunks = [x[SUB * q : SUB * q + SUB] for q in range(width // SUB)]
    for p in range(0, len(pieces), 2):
        pair = [x[a : a + 1] * chunks[q] for a, q in pieces[p : p + 2]]
        table_ref[SUB * p : SUB * (p + 2)] = jnp.concatenate(pair, axis=0).astype(jnp.bfloat16)


def three(x):
    high = x.astype(jnp.bfloat16)
    rest = x - high.astype(jnp.float32)
    mid = rest.astype(jnp.bfloat16)
    low = (rest - mid.astype(jnp.float32)).astype(jnp.bfloat16)
    return high, mid, low


def pad_rows(rows):
    index = lax.broadcasted_iota(jnp.int32, (16, rows[0].shape[1]), 0)
    total = jnp.zeros((16, rows[0].shape[1]), jnp.float32)
    for k, row in enumerate(rows):
        total = jnp.where(index == k, row.astype(jnp.float32), total)
    return total.astype(jnp.bfloat16)


def stack_left(x, offset):
    high, mid, low = three(x)
    return jnp.concatenate([high, mid, high, low, mid, high, pad_rows(list(three(offset)))], axis=0)


def stack_right(y):
    high, mid, low = three(y)
    ones = pad_rows([jnp.ones((1, y.shape[1]), jnp.float32)] * 3)
    return jnp.concatenate([high, high, mid, high, mid, low, ones], axis=0)


def cholesky_columns(get, put, width, lanes):
    blocks = width // SUB
    index = lax.broadcasted_iota(jnp.int32, (SUB, lanes), 0)
    trace = jnp.zeros((SUB, lanes), jnp.float32)
    for k in range(width):
        trace = trace + jnp.where(index == k % SUB, get(k, k // SUB), 0.0)
    shift = RIDGE + DAMPING / width * jnp.sum(trace, axis=0, keepdims=True)
    scales = []
    columns = []
    for k in range(width):
        first = k // SUB
        column = {q: get(k, q) for q in range(first, blocks)}
        column[first] = column[first] + jnp.where(index == k % SUB, shift, 0.0)
        for m in range(k):
            factor = columns[m][first][k % SUB : k % SUB + 1]
            for q in range(first, blocks):
                column[q] = column[q] - columns[m][q] * factor
        scale = lax.rsqrt(column[first][k % SUB : k % SUB + 1])
        column = {q: v * scale for q, v in column.items()}
        for q, v in column.items():
            put(k, q, v)
        columns.append(column)
        scales.append(scale)
    return columns, scales


def cholesky_substitute(columns, scales, right, width, lanes):
    blocks = width // SUB
    index = lax.broadcasted_iota(jnp.int32, (SUB, lanes), 0)
    right = list(right)
    forward = []
    for k in range(width):
        first = k // SUB
        value = right[first][k % SUB : k % SUB + 1] * scales[k]
        forward.append(value)
        for q in range(first, blocks):
            right[q] = right[q] - columns[k][q] * value
    answer = [jnp.zeros((SUB, lanes), jnp.float32)] * blocks
    for k in reversed(range(width)):
        first = k // SUB
        terms = sum(columns[k][q] * answer[q] for q in range(first, blocks))
        value = (forward[k] - jnp.sum(terms, axis=0, keepdims=True)) * scales[k]
        answer[first] = jnp.where(index == k % SUB, value, answer[first])
    return answer


def factor_moments_kernel(width, counts_ref, totals_ref, ut_ref, vt_ref, mine_ref, theirs_ref, keep_ref, table_ref):
    half = ut_ref.shape[1] // 2
    core = lax.rem(lax.axis_index("gene"), 2)
    parts = (pl.multiple_of(core * half, half), pl.multiple_of((1 - core) * half, half))
    offset = jnp.log(totals_ref[...].astype(jnp.float32)) - math.log(SCALE_TOTAL)
    keep_ref[...] = jnp.zeros_like(keep_ref)
    keep_ref[0:1] = offset
    vt = vt_ref[...]
    fill_table(table_ref, vt, width)
    right = stack_right(vt)
    low = vt.astype(jnp.bfloat16)
    across = (((1,), (1,)), ((), ()))
    for part, out_ref in zip(parts, (mine_ref, theirs_ref)):
        left = stack_left(ut_ref[:, pl.ds(part, half)], keep_ref[0:1, pl.ds(part, half)])
        linear = lax.dot_general(
            left, right, (((0,), (0,)), ((), ())), preferred_element_type=jnp.float32
        )
        expected = jnp.exp(linear)
        weights = expected.astype(jnp.bfloat16)
        counts = counts_ref[pl.ds(part, half), :].astype(jnp.float32)
        residual = (counts - expected).astype(jnp.bfloat16)
        rows = table_ref.shape[0]
        out_ref[:rows] = lax.dot_general(table_ref[...], weights, across, preferred_element_type=jnp.float32)
        out_ref[rows:] = lax.dot_general(low, residual, across, preferred_element_type=jnp.float32)


def factor_solve_kernel(width, own_ref, other_ref, totals_ref, ut_ref, new_ref):
    half = own_ref.shape[1]
    core = lax.rem(lax.axis_index("gene"), 2)
    part = pl.multiple_of(core * half, half)
    pieces = table_pieces(width)
    place = {piece: SUB * p for p, piece in enumerate(pieces)}
    base = SUB * len(pieces)

    def get(a, q):
        at = place[a, q]
        return own_ref[at : at + SUB, :] + other_ref[at : at + SUB, :]

    ut = ut_ref[:, pl.ds(part, half)]
    right = []
    for q in range(width // SUB):
        at = base + SUB * q
        gradient = own_ref[at : at + SUB, :] + other_ref[at : at + SUB, :]
        right.append(gradient - RIDGE * ut[SUB * q : SUB * q + SUB])
    columns, scales = cholesky_columns(get, lambda a, q, v: None, width, half)
    step = cholesky_substitute(columns, scales, right, width, half)
    offset = jnp.log(totals_ref[:, pl.ds(part, half)].astype(jnp.float32)) - math.log(SCALE_TOTAL)
    new_ref[...] = jnp.zeros_like(new_ref)
    for q in range(width // SUB):
        new_ref[0, SUB * q : SUB * q + SUB, :] = ut[SUB * q : SUB * q + SUB] + step[q]
    new_ref[0, width : width + 1, :] = offset


def counts_kernel(width, counts_ref, mine_ref, theirs_ref, vt_ref, factors_ref, linear_ref):
    half = mine_ref.shape[2]
    core = lax.rem(lax.axis_index("gene"), 2)
    total = jnp.zeros((width, counts_ref.shape[1]), jnp.float32)
    terms = jnp.zeros((1, counts_ref.shape[1]), jnp.float32)
    for own, block_ref in ((1, mine_ref), (0, theirs_ref)):
        index = core if own else 1 - core
        part = pl.multiple_of(index * half, half)
        block = block_ref[0]
        factors = block[:width]
        factors_ref[:, pl.ds(part, half)] = factors
        counts = counts_ref[pl.ds(part, half), :].astype(jnp.float32)
        exact = counts.astype(jnp.bfloat16)
        high, mid, low = three(factors)
        both = jnp.concatenate([high, mid, low], axis=0)
        product = jnp.dot(both, exact, preferred_element_type=jnp.float32)
        total = total + product[:width]
        full = product[:width] + (product[width : 2 * width] + product[2 * width :])
        terms = terms - jnp.sum(full * vt_ref[...], axis=0, keepdims=True)
        oh, om, ol = three(block[width : width + 1])
        offsets = jnp.dot(pad_rows([oh, om, ol]), exact, preferred_element_type=jnp.float32)
        own_terms = counts * (jnp.log(jnp.maximum(counts, 1.0)) - 1.0)
        terms = terms + jnp.sum(own_terms, axis=0, keepdims=True)
        terms = terms - jnp.sum(offsets[:SUB], axis=0, keepdims=True)
    linear_ref[:width] = total
    linear_ref[width:] = jnp.zeros_like(linear_ref[width:])
    linear_ref[width : width + 1] = terms


def loading_moments_kernel(width, chunk, tile, mine_ref, theirs_ref, vt_ref, out_ref, sum_ref, table_ref, left_ref, right_ref):
    genes = vt_ref.shape[1]
    half = mine_ref.shape[2]
    blocks = mine_ref.shape[0]
    per = chunk // half
    rows = SUB * len(table_pieces(width))
    out_ref[...] = jnp.zeros_like(out_ref)
    sum_ref[...] = jnp.zeros_like(sum_ref)
    right_ref[...] = stack_right(vt_ref[...])

    for block_ref in (mine_ref, theirs_ref):

        @pl.loop(0, blocks // per)
        def _(group):
            for b in range(per):
                block = block_ref[group * per + b]
                factors = block[:width]
                cols = slice(b * half, (b + 1) * half)
                fill_table(table_ref.at[:, cols], factors, width)
                table_ref[rows : rows + width, cols] = factors.astype(jnp.bfloat16)
                left_ref[:, cols] = stack_left(factors, block[width : width + 1])

            @pl.loop(0, genes // tile)
            def _(j):
                at = pl.ds(pl.multiple_of(j * tile, tile), tile)
                linear = lax.dot_general(
                    left_ref[...], right_ref[:, at], (((0,), (0,)), ((), ())), preferred_element_type=jnp.float32
                )
                expected = jnp.exp(linear)
                sum_ref[0:1, at] += jnp.sum(expected, axis=0, keepdims=True)
                weights = expected.astype(jnp.bfloat16)
                out_ref[:, at] += jnp.dot(table_ref[...], weights, preferred_element_type=jnp.float32)


def loading_solve_kernel(width, tile, total_cells, moments_ref, sum_ref, own_ref, other_ref, vt_ref, new_ref, deviance_ref, lower_ref):
    genes = vt_ref.shape[1]
    pieces = table_pieces(width)
    place = {piece: SUB * p for p, piece in enumerate(pieces)}
    base = SUB * len(pieces)
    blocks = width // SUB

    @pl.loop(0, genes // tile)
    def _(j):
        at = pl.ds(pl.multiple_of(j * tile, tile), tile)

        def get(a, q):
            return moments_ref[place[a, q] : place[a, q] + SUB, at]

        vt = [vt_ref[SUB * q : SUB * q + SUB, at] for q in range(blocks)]
        seen = [
            own_ref[SUB * q : SUB * q + SUB, at] + other_ref[SUB * q : SUB * q + SUB, at] for q in range(blocks + 1)
        ]
        right = []
        for q in range(blocks):
            right.append(seen[q] - moments_ref[base + SUB * q : base + SUB * q + SUB, at] - RIDGE * vt[q])
        columns, scales = cholesky_columns(get, lambda a, q, v: None, width, tile)
        step = cholesky_substitute(columns, scales, right, width, tile)
        for q in range(blocks):
            new_ref[SUB * q : SUB * q + SUB, at] = vt[q] + step[q]
        fixed = seen[blocks][0:1] + sum_ref[0:1, at]
        deviance_ref[:, at] = fixed * (2.0 / total_cells)


def kernel_call(body, outs, scratch, name, flops):
    single = pl.BlockSpec(memory_space=pltpu.VMEM)

    def call(*args):
        return pl.pallas_call(
            body,
            out_shape=outs,
            in_specs=[single] * len(args),
            out_specs=jax.tree.map(lambda _: single, outs),
            scratch_shapes=scratch,
            compiler_params=pltpu.CompilerParams(vmem_limit_bytes=VMEM_LIMIT),
            cost_estimate=pl.CostEstimate(flops=flops, bytes_accessed=1 << 20, transcendentals=0),
            name=name,
        )(*args)

    return call


def exchange(x, axis, bit):
    size = lax.axis_size(axis)
    return lax.ppermute(x, axis, [(i, i ^ bit) for i in range(size)])


def on_device(counts, totals, cell_factors, gene_loadings):
    cells, genes = counts.shape
    width = cell_factors.shape[1]
    half = cells // 2
    rows = SUB * len(table_pieces(width))
    shape = functools.partial(jax.ShapeDtypeStruct, dtype=jnp.float32)
    tall = width + SUB
    ut, vt = cell_factors.T, gene_loadings.T
    totals = totals.reshape(1, cells)

    mine, theirs = kernel_call(
        functools.partial(factor_moments_kernel, width),
        (shape((rows + width, half)), shape((rows + width, half))),
        [pltpu.VMEM((SUB, cells), jnp.float32), pltpu.VMEM((rows, genes), jnp.bfloat16)],
        "factor_moments",
        10**9,
    )(counts, totals, ut, vt)
    mine = mine + exchange(theirs, "gene", 1)
    bits = [1 << k for k in range(1, (lax.axis_size("gene") - 1).bit_length())]
    for bit in bits[:-1]:
        mine = mine + exchange(mine, "gene", bit)
    other = exchange(mine, "gene", bits[-1])
    block = kernel_call(
        functools.partial(factor_solve_kernel, width), shape((1, tall, half)), [], "factor_solve", 10**9
    )(mine, other, totals, ut)

    partner = exchange(block, "gene", 1)
    cell_bits = [1 << k for k in range((lax.axis_size("cell") - 1).bit_length())]
    gathered = block
    for bit in reversed(cell_bits):
        gathered = jnp.concatenate([gathered, exchange(gathered, "cell", bit)], axis=0)
    opposite = exchange(gathered, "gene", 1)

    factors, linear = kernel_call(
        functools.partial(counts_kernel, width), (shape((width, cells)), shape((tall, genes))), [], "counts", 10**8
    )(counts, block, partner, vt)
    for bit in cell_bits[:-1]:
        linear = linear + exchange(linear, "cell", bit)
    linear_other = exchange(linear, "cell", cell_bits[-1])

    chunk = min(gathered.shape[0], 8) * half
    tile = 256
    depth = 6 * width + 16
    moments, sums = kernel_call(
        functools.partial(loading_moments_kernel, width, chunk, tile),
        (shape((rows + width, genes)), shape((SUB, genes))),
        [
            pltpu.VMEM((rows + width, chunk), jnp.bfloat16),
            pltpu.VMEM((depth, chunk), jnp.bfloat16),
            pltpu.VMEM((depth, genes), jnp.bfloat16),
        ],
        "loading_moments",
        4 * 10**9,
    )(gathered, opposite, vt)
    total_cells = cells * lax.axis_size("cell")
    new_loadings, deviance = kernel_call(
        functools.partial(loading_solve_kernel, width, 256, total_cells),
        (shape((width, genes)), shape((1, genes))),
        [pltpu.VMEM((rows, 256), jnp.float32)],
        "loading_solve",
        10**9,
    )(moments, sums, linear, linear_other, vt)
    return (factors.T, new_loadings.T, deviance.reshape(genes))


def solution(mesh):
    return jax.shard_map(
        on_device,
        mesh=mesh,
        in_specs=(P("cell", "gene"), P("cell"), P("cell", None), P("gene", None)),
        out_specs=(P("cell", None), P("gene", None), P("gene")),
        check_vma=False,
    )
```

```python
import functools
import math

import jax
import jax.numpy as jnp
from jax import lax
from jax.experimental import pallas as pl
from jax.experimental.pallas import tpu as pltpu
from jax.sharding import PartitionSpec as P


RIDGE = 1.0
DAMPING = 0.1
SCALE_TOTAL = 5000.0
SUB = 8
MIB = 1024 * 1024


def table_pieces(width):
    return [(a, q) for a in range(width) for q in range(a // SUB, width // SUB)]


def fill_table(table_ref, x, width):
    pieces = table_pieces(width)
    chunks = [x[SUB * q : SUB * q + SUB] for q in range(width // SUB)]
    for p in range(0, len(pieces), 2):
        pair = [x[a : a + 1] * chunks[q] for a, q in pieces[p : p + 2]]
        table_ref[SUB * p : SUB * (p + 2)] = jnp.concatenate(pair, axis=0).astype(jnp.bfloat16)


def three(x):
    high = x.astype(jnp.bfloat16)
    rest = x - high.astype(jnp.float32)
    mid = rest.astype(jnp.bfloat16)
    low = (rest - mid.astype(jnp.float32)).astype(jnp.bfloat16)
    return high, mid, low


def pad_rows(rows):
    index = lax.broadcasted_iota(jnp.int32, (16, rows[0].shape[1]), 0)
    total = jnp.zeros((16, rows[0].shape[1]), jnp.float32)
    for k, row in enumerate(rows):
        total = jnp.where(index == k, row.astype(jnp.float32), total)
    return total.astype(jnp.bfloat16)


def stack_left(x, offset):
    high, mid, low = three(x)
    return jnp.concatenate([high, mid, high, low, mid, high, pad_rows(list(three(offset)))], axis=0)


def stack_right(y):
    high, mid, low = three(y)
    ones = pad_rows([jnp.ones((1, y.shape[1]), jnp.float32)] * 3)
    return jnp.concatenate([high, high, mid, high, mid, low, ones], axis=0)


def cholesky_columns(get, put, width, lanes):
    blocks = width // SUB
    index = lax.broadcasted_iota(jnp.int32, (SUB, lanes), 0)
    trace = jnp.zeros((SUB, lanes), jnp.float32)
    for k in range(width):
        trace = trace + jnp.where(index == k % SUB, get(k, k // SUB), 0.0)
    shift = RIDGE + DAMPING / width * jnp.sum(trace, axis=0, keepdims=True)
    scales = []
    columns = []
    for k in range(width):
        first = k // SUB
        column = {q: get(k, q) for q in range(first, blocks)}
        column[first] = column[first] + jnp.where(index == k % SUB, shift, 0.0)
        for m in range(k):
            factor = columns[m][first][k % SUB : k % SUB + 1]
            for q in range(first, blocks):
                column[q] = column[q] - columns[m][q] * factor
        scale = lax.rsqrt(column[first][k % SUB : k % SUB + 1])
        column = {q: v * scale for q, v in column.items()}
        for q, v in column.items():
            put(k, q, v)
        columns.append(column)
        scales.append(scale)
    return columns, scales


def cholesky_substitute(columns, scales, right, width, lanes):
    blocks = width // SUB
    index = lax.broadcasted_iota(jnp.int32, (SUB, lanes), 0)
    right = list(right)
    forward = []
    for k in range(width):
        first = k // SUB
        value = right[first][k % SUB : k % SUB + 1] * scales[k]
        forward.append(value)
        for q in range(first, blocks):
            right[q] = right[q] - columns[k][q] * value
    answer = [jnp.zeros((SUB, lanes), jnp.float32)] * blocks
    for k in reversed(range(width)):
        first = k // SUB
        terms = sum(columns[k][q] * answer[q] for q in range(first, blocks))
        value = (forward[k] - jnp.sum(terms, axis=0, keepdims=True)) * scales[k]
        answer[first] = jnp.where(index == k % SUB, value, answer[first])
    return answer


def factor_moments_kernel(width, counts_ref, totals_ref, ut_ref, vt_ref, mine_ref, theirs_ref, keep_ref, table_ref):
    half = ut_ref.shape[1] // 2
    core = lax.rem(lax.axis_index("gene"), 2)
    parts = (pl.multiple_of(core * half, half), pl.multiple_of((1 - core) * half, half))
    offset = jnp.log(totals_ref[...].astype(jnp.float32)) - math.log(SCALE_TOTAL)
    keep_ref[...] = jnp.zeros_like(keep_ref)
    keep_ref[0:1] = offset
    vt = vt_ref[...]
    fill_table(table_ref, vt, width)
    right = stack_right(vt)
    low = vt.astype(jnp.bfloat16)
    across = (((1,), (1,)), ((), ()))
    for part, out_ref in zip(parts, (mine_ref, theirs_ref)):
        left = stack_left(ut_ref[:, pl.ds(part, half)], keep_ref[0:1, pl.ds(part, half)])
        linear = lax.dot_general(
            left, right, (((0,), (0,)), ((), ())), preferred_element_type=jnp.float32
        )
        expected = jnp.exp(linear)
        weights = expected.astype(jnp.bfloat16)
        counts = counts_ref[pl.ds(part, half), :].astype(jnp.float32)
        residual = (counts - expected).astype(jnp.bfloat16)
        rows = table_ref.shape[0]
        out_ref[:rows] = lax.dot_general(table_ref[...], weights, across, preferred_element_type=jnp.float32)
        out_ref[rows:] = lax.dot_general(low, residual, across, preferred_element_type=jnp.float32)


def factor_solve_kernel(width, own_ref, other_ref, totals_ref, ut_ref, new_ref):
    half = own_ref.shape[1]
    core = lax.rem(lax.axis_index("gene"), 2)
    part = pl.multiple_of(core * half, half)
    pieces = table_pieces(width)
    place = {piece: SUB * p for p, piece in enumerate(pieces)}
    base = SUB * len(pieces)

    def get(a, q):
        at = place[a, q]
        return own_ref[at : at + SUB, :] + other_ref[at : at + SUB, :]

    ut = ut_ref[:, pl.ds(part, half)]
    right = []
    for q in range(width // SUB):
        at = base + SUB * q
        gradient = own_ref[at : at + SUB, :] + other_ref[at : at + SUB, :]
        right.append(gradient - RIDGE * ut[SUB * q : SUB * q + SUB])
    columns, scales = cholesky_columns(get, lambda a, q, v: None, width, half)
    step = cholesky_substitute(columns, scales, right, width, half)
    offset = jnp.log(totals_ref[:, pl.ds(part, half)].astype(jnp.float32)) - math.log(SCALE_TOTAL)
    new_ref[...] = jnp.zeros_like(new_ref)
    for q in range(width // SUB):
        new_ref[0, SUB * q : SUB * q + SUB, :] = ut[SUB * q : SUB * q + SUB] + step[q]
    new_ref[0, width : width + 1, :] = offset


def counts_kernel(width, counts_ref, mine_ref, theirs_ref, vt_ref, factors_ref, linear_ref):
    half = mine_ref.shape[2]
    core = lax.rem(lax.axis_index("gene"), 2)
    total = jnp.zeros((width, counts_ref.shape[1]), jnp.float32)
    terms = jnp.zeros((1, counts_ref.shape[1]), jnp.float32)
    for own, block_ref in ((1, mine_ref), (0, theirs_ref)):
        index = core if own else 1 - core
        part = pl.multiple_of(index * half, half)
        block = block_ref[0]
        factors = block[:width]
        factors_ref[:, pl.ds(part, half)] = factors
        counts = counts_ref[pl.ds(part, half), :].astype(jnp.float32)
        exact = counts.astype(jnp.bfloat16)
        high, mid, low = three(factors)
        both = jnp.concatenate([high, mid, low], axis=0)
        product = jnp.dot(both, exact, preferred_element_type=jnp.float32)
        total = total + product[:width]
        full = product[:width] + (product[width : 2 * width] + product[2 * width :])
        terms = terms - jnp.sum(full * vt_ref[...], axis=0, keepdims=True)
        oh, om, ol = three(block[width : width + 1])
        offsets = jnp.dot(pad_rows([oh, om, ol]), exact, preferred_element_type=jnp.float32)
        own_terms = counts * (jnp.log(jnp.maximum(counts, 1.0)) - 1.0)
        terms = terms + jnp.sum(own_terms, axis=0, keepdims=True)
        terms = terms - jnp.sum(offsets[:SUB], axis=0, keepdims=True)
    linear_ref[:width] = total
    linear_ref[width:] = jnp.zeros_like(linear_ref[width:])
    linear_ref[width : width + 1] = terms


def loading_moments_kernel(width, per, tile, blocks_ref, vt_ref, out_ref, sum_ref, table_ref, left_ref, right_ref):
    genes = vt_ref.shape[1]
    half = blocks_ref.shape[2]
    groups = blocks_ref.shape[0] // per
    rows = SUB * len(table_pieces(width))
    right_ref[...] = stack_right(vt_ref[...])
    if groups > 1:
        out_ref[...] = jnp.zeros_like(out_ref)
        sum_ref[...] = jnp.zeros_like(sum_ref)

    @pl.loop(0, groups)
    def _(group):
        for b in range(per):
            block = blocks_ref[group * per + b]
            factors = block[:width]
            cols = slice(b * half, (b + 1) * half)
            fill_table(table_ref.at[:, cols], factors, width)
            table_ref[rows : rows + width, cols] = factors.astype(jnp.bfloat16)
            left_ref[:, cols] = stack_left(factors, block[width : width + 1])

        @pl.loop(0, genes // tile)
        def _(j):
            at = pl.ds(pl.multiple_of(j * tile, tile), tile)
            linear = lax.dot_general(
                left_ref[...], right_ref[:, at], (((0,), (0,)), ((), ())), preferred_element_type=jnp.float32
            )
            expected = jnp.exp(linear)
            total = jnp.sum(expected, axis=0, keepdims=True)
            product = jnp.dot(table_ref[...], expected.astype(jnp.bfloat16), preferred_element_type=jnp.float32)
            if groups > 1:
                sum_ref[0:1, at] += total
                out_ref[:, at] += product
            else:
                sum_ref[0:1, at] = total
                out_ref[:, at] = product


def loading_factor_kernel(width, tile, moments_ref, more_ref, lower_ref, scale_ref):
    genes = moments_ref.shape[1]
    place = {piece: SUB * p for p, piece in enumerate(table_pieces(width))}

    @pl.loop(0, genes // tile)
    def _(j):
        at = pl.ds(pl.multiple_of(j * tile, tile), tile)

        def get(a, q):
            rows = slice(place[a, q], place[a, q] + SUB)
            return moments_ref[rows, at] + more_ref[rows, at]

        def put(a, q, value):
            lower_ref[place[a, q] : place[a, q] + SUB, at] = value

        _, scales = cholesky_columns(get, put, width, tile)
        for k in range(width):
            scale_ref[k : k + 1, at] = scales[k]


def loading_solve_kernel(width, tile, total_cells, lower_ref, scale_ref, moments_ref, more_ref, sum_ref, sums_ref, own_ref, other_ref, vt_ref, new_ref, deviance_ref):
    genes = vt_ref.shape[1]
    place = {piece: SUB * p for p, piece in enumerate(table_pieces(width))}
    base = SUB * len(place)
    blocks = width // SUB

    @pl.loop(0, genes // tile)
    def _(j):
        at = pl.ds(pl.multiple_of(j * tile, tile), tile)
        right = []
        for q in range(blocks):
            rows = slice(SUB * q, SUB * q + SUB)
            expected = moments_ref[base + SUB * q : base + SUB * q + SUB, at]
            expected = expected + more_ref[base + SUB * q : base + SUB * q + SUB, at]
            right.append(own_ref[rows, at] + other_ref[rows, at] - expected - RIDGE * vt_ref[rows, at])
        columns = [
            {q: lower_ref[place[k, q] : place[k, q] + SUB, at] for q in range(k // SUB, blocks)} for k in range(width)
        ]
        scales = [scale_ref[k : k + 1, at] for k in range(width)]
        step = cholesky_substitute(columns, scales, right, width, tile)
        for q in range(blocks):
            rows = slice(SUB * q, SUB * q + SUB)
            new_ref[rows, at] = vt_ref[rows, at] + step[q]
        last = slice(width, width + 1)
        fixed = own_ref[last, at] + other_ref[last, at] + sum_ref[0:1, at] + sums_ref[0:1, at]
        deviance_ref[:, at] = fixed * (2.0 / total_cells)


def kernel_call(body, outs, scratch, flops, limit=8):
    single = pl.BlockSpec(memory_space=pltpu.VMEM)

    def call(*args):
        return pl.pallas_call(
            body,
            out_shape=outs,
            in_specs=[single] * len(args),
            out_specs=jax.tree.map(lambda _: single, outs),
            scratch_shapes=scratch,
            compiler_params=pltpu.CompilerParams(vmem_limit_bytes=limit * MIB),
            cost_estimate=pl.CostEstimate(flops=flops, bytes_accessed=1 << 20, transcendentals=0),
        )(*args)

    return call


def exchange(x, axis, bit):
    size = lax.axis_size(axis)
    return lax.ppermute(x, axis, [(i, i ^ bit) for i in range(size)])


def sweep(counts, totals, cell_factors, gene_loadings):
    cells, genes = counts.shape
    width = cell_factors.shape[1]
    half = cells // 2
    rows = SUB * len(table_pieces(width))
    shape = functools.partial(jax.ShapeDtypeStruct, dtype=jnp.float32)
    tall = width + SUB
    ut, vt = cell_factors.T, gene_loadings.T
    totals = totals.reshape(1, cells)

    mine, theirs = kernel_call(
        functools.partial(factor_moments_kernel, width),
        (shape((rows + width, half)), shape((rows + width, half))),
        [pltpu.VMEM((SUB, cells), jnp.float32), pltpu.VMEM((rows, genes), jnp.bfloat16)],
        10**9,
    )(counts, totals, ut, vt)
    mine = mine + exchange(theirs, "gene", 1)
    bits = [1 << k for k in range(1, (lax.axis_size("gene") - 1).bit_length())]
    for bit in bits[:-1]:
        mine = mine + exchange(mine, "gene", bit)
    other = exchange(mine, "gene", bits[-1])
    block = kernel_call(
        functools.partial(factor_solve_kernel, width), shape((1, tall, half)), [], 10**9
    )(mine, other, totals, ut)

    cell_bits = [1 << k for k in range((lax.axis_size("cell") - 1).bit_length())]
    gathered = block
    for bit in reversed(cell_bits):
        gathered = jnp.concatenate([gathered, exchange(gathered, "cell", bit)], axis=0)
    partner = exchange(block, "gene", 1)
    opposite = exchange(gathered, "gene", 1)

    factors, linear = kernel_call(
        functools.partial(counts_kernel, width), (shape((width, cells)), shape((tall, genes))), [], 10**9
    )(counts, block, partner, vt)
    for bit in cell_bits[:-1]:
        linear = linear + exchange(linear, "cell", bit)
    linear_other = exchange(linear, "cell", cell_bits[-1])

    per = min(gathered.shape[0], 8)
    tile = 256
    depth = 6 * width + 16

    def moments_of(blocks):
        return kernel_call(
            functools.partial(loading_moments_kernel, width, per, tile),
            (shape((rows + width, genes)), shape((SUB, genes))),
            [
                pltpu.VMEM((rows + width, per * half), jnp.bfloat16),
                pltpu.VMEM((depth, per * half), jnp.bfloat16),
                pltpu.VMEM((depth, genes), jnp.bfloat16),
            ],
            4 * 10**9,
            16,
        )(blocks, vt)

    moments, sums = moments_of(gathered)
    more, more_sums = moments_of(opposite)
    lower, scales = kernel_call(
        functools.partial(loading_factor_kernel, width, 256),
        (shape((rows, genes)), shape((width, genes))),
        [],
        4 * 10**9,
    )(moments, more)
    total_cells = cells * lax.axis_size("cell")
    new_loadings, deviance = kernel_call(
        functools.partial(loading_solve_kernel, width, min(genes, 1024), total_cells),
        (shape((width, genes)), shape((1, genes))),
        [],
        10**9,
    )(lower, scales, moments, more, sums, more_sums, linear, linear_other, vt)
    return (factors.T, new_loadings.T, deviance.reshape(genes))


def solution(mesh):
    return jax.shard_map(
        sweep,
        mesh=mesh,
        in_specs=(P("cell", "gene"), P("cell"), P("cell", None), P("gene", None)),
        out_specs=(P("cell", None), P("gene", None), P("gene")),
        check_vma=False,
    )
```

```python
import functools
import math

import jax
import jax.numpy as jnp
from jax import lax
from jax.experimental import pallas as pl
from jax.experimental.pallas import tpu as pltpu
from jax.sharding import PartitionSpec as P


RIDGE = 1.0
DAMPING = 0.1
SCALE_TOTAL = 5000.0
SUB = 8
LANES = 128
MIB = 1024 * 1024


def table_pieces(width):
    return [(a, q) for a in range(width) for q in range(a // SUB, width // SUB)]


def fill_table(table_ref, x, width):
    pieces = table_pieces(width)
    chunks = [x[SUB * q : SUB * q + SUB] for q in range(width // SUB)]
    for p in range(0, len(pieces), 2):
        pair = [x[a : a + 1] * chunks[q] for a, q in pieces[p : p + 2]]
        table_ref[SUB * p : SUB * (p + 2)] = jnp.concatenate(pair, axis=0).astype(jnp.bfloat16)


def three(x):
    high = x.astype(jnp.bfloat16)
    rest = x - high.astype(jnp.float32)
    mid = rest.astype(jnp.bfloat16)
    low = (rest - mid.astype(jnp.float32)).astype(jnp.bfloat16)
    return high, mid, low


def pad_rows(rows):
    index = lax.broadcasted_iota(jnp.int32, (16, rows[0].shape[1]), 0)
    total = jnp.zeros((16, rows[0].shape[1]), jnp.float32)
    for k, row in enumerate(rows):
        total = jnp.where(index == k, row.astype(jnp.float32), total)
    return total.astype(jnp.bfloat16)


def stack_left(x, offset):
    high, mid, low = three(x)
    return jnp.concatenate([high, mid, high, low, mid, high, pad_rows(list(three(offset)))], axis=0)


def stack_right(y):
    high, mid, low = three(y)
    ones = pad_rows([jnp.ones((1, y.shape[1]), jnp.float32)] * 3)
    return jnp.concatenate([high, high, mid, high, mid, low, ones], axis=0)


def cholesky_columns(get, put, width, lanes):
    blocks = width // SUB
    index = lax.broadcasted_iota(jnp.int32, (SUB, lanes), 0)
    trace = jnp.zeros((SUB, lanes), jnp.float32)
    for k in range(width):
        trace = trace + jnp.where(index == k % SUB, get(k, k // SUB), 0.0)
    shift = RIDGE + DAMPING / width * jnp.sum(trace, axis=0, keepdims=True)
    scales = []
    columns = []
    for k in range(width):
        first = k // SUB
        column = {q: get(k, q) for q in range(first, blocks)}
        column[first] = column[first] + jnp.where(index == k % SUB, shift, 0.0)
        for m in range(k):
            factor = columns[m][first][k % SUB : k % SUB + 1]
            for q in range(first, blocks):
                column[q] = column[q] - columns[m][q] * factor
        scale = lax.rsqrt(column[first][k % SUB : k % SUB + 1])
        column = {q: v * scale for q, v in column.items()}
        for q, v in column.items():
            put(k, q, v)
        columns.append(column)
        scales.append(scale)
    return columns, scales


def cholesky_substitute(columns, scales, right, width, lanes):
    blocks = width // SUB
    index = lax.broadcasted_iota(jnp.int32, (SUB, lanes), 0)
    right = list(right)
    forward = []
    for k in range(width):
        first = k // SUB
        value = right[first][k % SUB : k % SUB + 1] * scales[k]
        forward.append(value)
        for q in range(first, blocks):
            right[q] = right[q] - columns[k][q] * value
    answer = [jnp.zeros((SUB, lanes), jnp.float32)] * blocks
    for k in reversed(range(width)):
        first = k // SUB
        terms = sum(columns[k][q] * answer[q] for q in range(first, blocks))
        value = (forward[k] - jnp.sum(terms, axis=0, keepdims=True)) * scales[k]
        answer[first] = jnp.where(index == k % SUB, value, answer[first])
    return answer


def halves(ref):
    half = ref.shape[1] // 2
    core = lax.rem(lax.axis_index("gene"), 2)
    return [ref[:, pl.ds(pl.multiple_of(index * half, half), half)] for index in (core, 1 - core)]


def factor_gradient_kernel(counts_hbm, totals_hbm, ut_hbm, vt_hbm, mine_ref, theirs_ref, exact_ref, offset_ref, ut_ref, vt_ref, counts_ref, totals_ref, sems):
    copies = [
        pltpu.make_async_copy(source, target, sems.at[k])
        for k, (source, target) in enumerate(
            ((totals_hbm, totals_ref), (ut_hbm, ut_ref), (vt_hbm, vt_ref), (counts_hbm, counts_ref))
        )
    ]
    for copy in copies:
        copy.start()
    for copy in copies[:3]:
        copy.wait()
    half = ut_ref.shape[1] // 2
    core = lax.rem(lax.axis_index("gene"), 2)
    offset_ref[...] = jnp.log(totals_ref[...].astype(jnp.float32)) - math.log(SCALE_TOTAL)
    vt = vt_ref[...]
    right = stack_right(vt)
    low = vt.astype(jnp.bfloat16)
    linear = [
        lax.dot_general(stack_left(ut, offset), right, (((0,), (0,)), ((), ())), preferred_element_type=jnp.float32)
        for ut, offset in zip(halves(ut_ref), halves(offset_ref))
    ]
    copies[3].wait()
    for index, lin, out_ref in ((core, linear[0], mine_ref), (1 - core, linear[1], theirs_ref)):
        part = pl.ds(pl.multiple_of(index * half, half), half)
        counts = counts_ref[part, :].astype(jnp.float32)
        exact_ref[part, :] = counts.astype(jnp.bfloat16)
        residual = (counts - jnp.exp(lin)).astype(jnp.bfloat16)
        out_ref[...] = lax.dot_general(low, residual, (((1,), (1,)), ((), ())), preferred_element_type=jnp.float32)


def factor_moments_kernel(width, add, *refs):
    (vt_ref, offset_ref, ut_ref), before, (mine_ref, theirs_ref, table_ref) = refs[:3], refs[3:-3], refs[-3:]
    half = ut_ref.shape[1] // 2
    vt = vt_ref[...]
    fill_table(table_ref, vt, width)
    left = [stack_left(ut, offset) for ut, offset in zip(halves(ut_ref), halves(offset_ref))]
    linear = lax.dot_general(
        stack_right(vt), jnp.concatenate(left, axis=1), (((0,), (0,)), ((), ())), preferred_element_type=jnp.float32
    )
    weights = jnp.exp(linear).astype(jnp.bfloat16)
    product = jnp.dot(table_ref[...], weights, preferred_element_type=jnp.float32)
    for k, out_ref in enumerate((mine_ref, theirs_ref)):
        total = product[:, k * half : (k + 1) * half]
        if add:
            total = total + before[k][...]
        out_ref[...] = total


def factor_solve_kernel(width, terms, *refs):
    moments, (own_ref, other_ref, offset_ref, ut_ref, new_ref) = refs[:terms], refs[terms:]
    half = own_ref.shape[1]
    place = {piece: SUB * p for p, piece in enumerate(table_pieces(width))}

    def get(a, q):
        at = place[a, q]
        return sum(ref[at : at + SUB, :] for ref in moments)

    ut = halves(ut_ref)[0]
    right = []
    for q in range(width // SUB):
        rows = slice(SUB * q, SUB * q + SUB)
        right.append(own_ref[rows] + other_ref[rows] - RIDGE * ut[rows])
    columns, scales = cholesky_columns(get, lambda a, q, v: None, width, half)
    step = cholesky_substitute(columns, scales, right, width, half)
    new_ref[...] = jnp.zeros_like(new_ref)
    for q in range(width // SUB):
        new_ref[0, SUB * q : SUB * q + SUB, :] = ut[SUB * q : SUB * q + SUB] + step[q]
    new_ref[0, width : width + 1, :] = halves(offset_ref)[0]


def counts_kernel(width, exact_ref, mine_ref, theirs_ref, vt_ref, factors_ref, linear_ref):
    half = mine_ref.shape[2]
    genes = exact_ref.shape[1]
    core = lax.rem(lax.axis_index("gene"), 2)
    total = jnp.zeros((width, genes), jnp.float32)
    terms = jnp.zeros((1, genes), jnp.float32)
    for index, block_ref in ((core, mine_ref), (1 - core, theirs_ref)):
        part = pl.ds(pl.multiple_of(index * half, half), half)
        block = block_ref[0]
        factors = block[:width]
        factors_ref[:, part] = factors
        exact = exact_ref[part, :]
        high, mid, low = three(factors)
        both = jnp.concatenate([high, mid, low, pad_rows(list(three(block[width : width + 1])))], axis=0)
        product = jnp.dot(both, exact, preferred_element_type=jnp.float32)
        total = total + product[:width]
        full = product[:width] + (product[width : 2 * width] + product[2 * width : 3 * width])
        terms = terms - jnp.sum(full * vt_ref[...], axis=0, keepdims=True)
        terms = terms - jnp.sum(product[3 * width : 3 * width + SUB], axis=0, keepdims=True)
        counts = exact.astype(jnp.float32)
        own_terms = counts * (jnp.log(jnp.maximum(counts, 1.0)) - 1.0)
        terms = terms + jnp.sum(own_terms, axis=0, keepdims=True)
    groups = genes // LANES
    for j in range(groups):
        cols = slice(j * LANES, (j + 1) * LANES)
        linear_ref[width * j : width * (j + 1), :] = total[:, cols]
        linear_ref[width * groups + j : width * groups + j + 1, :] = terms[:, cols]


def loading_moments_kernel(width, per, tile, blocks_ref, vt_ref, out_ref, sum_ref, table_ref, left_ref, right_ref):
    genes = vt_ref.shape[1]
    half = blocks_ref.shape[2]
    groups = blocks_ref.shape[0] // per
    rows = SUB * len(table_pieces(width))
    right_ref[...] = stack_right(vt_ref[...])
    if groups > 1:
        out_ref[...] = jnp.zeros_like(out_ref)
        sum_ref[...] = jnp.zeros_like(sum_ref)

    @pl.loop(0, groups)
    def _(group):
        for b in range(per):
            block = blocks_ref[group * per + b]
            factors = block[:width]
            cols = slice(b * half, (b + 1) * half)
            fill_table(table_ref.at[:, cols], factors, width)
            table_ref[rows : rows + width, cols] = factors.astype(jnp.bfloat16)
            left_ref[:, cols] = stack_left(factors, block[width : width + 1])

        @pl.loop(0, genes // tile)
        def _(j):
            at = pl.ds(pl.multiple_of(j * tile, tile), tile)
            linear = lax.dot_general(
                left_ref[...], right_ref[:, at], (((0,), (0,)), ((), ())), preferred_element_type=jnp.float32
            )
            expected = jnp.exp(linear)
            total = jnp.sum(expected, axis=0, keepdims=True)
            product = jnp.dot(table_ref[...], expected.astype(jnp.bfloat16), preferred_element_type=jnp.float32)
            if groups > 1:
                sum_ref[0:1, at] += total
                out_ref[:, at] += product
            else:
                sum_ref[0:1, at] = total
                out_ref[:, at] = product


def loading_factor_kernel(width, tile, moments_ref, more_ref, lower_ref, scale_ref):
    genes = moments_ref.shape[1]
    place = {piece: SUB * p for p, piece in enumerate(table_pieces(width))}

    @pl.loop(0, genes // tile)
    def _(j):
        at = pl.ds(pl.multiple_of(j * tile, tile), tile)

        def get(a, q):
            rows = slice(place[a, q], place[a, q] + SUB)
            return moments_ref[rows, at] + more_ref[rows, at]

        def put(a, q, value):
            lower_ref[place[a, q] : place[a, q] + SUB, at] = value

        _, scales = cholesky_columns(get, put, width, tile)
        for k in range(width):
            scale_ref[k : k + 1, at] = scales[k]


def loading_solve_kernel(width, tile, total_cells, lower_ref, scale_ref, moments_ref, more_ref, sum_ref, sums_ref, own_ref, other_ref, vt_ref, new_ref, deviance_ref):
    genes = vt_ref.shape[1]
    place = {piece: SUB * p for p, piece in enumerate(table_pieces(width))}
    base = SUB * len(place)
    blocks = width // SUB

    groups = genes // LANES

    def seen(first, count):
        parts = [own_ref[f : f + count] + other_ref[f : f + count] for f in first]
        return jnp.concatenate(parts, axis=1)

    for j in range(genes // tile):
        at = slice(j * tile, (j + 1) * tile)
        lanes = range(j * tile // LANES, (j + 1) * tile // LANES)
        right = []
        for q in range(blocks):
            rows = slice(SUB * q, SUB * q + SUB)
            expected = moments_ref[base + SUB * q : base + SUB * q + SUB, at]
            expected = expected + more_ref[base + SUB * q : base + SUB * q + SUB, at]
            counted = seen([width * g + SUB * q for g in lanes], SUB)
            right.append(counted - expected - RIDGE * vt_ref[rows, at])
        columns = [
            {q: lower_ref[place[k, q] : place[k, q] + SUB, at] for q in range(k // SUB, blocks)} for k in range(width)
        ]
        scales = [scale_ref[k : k + 1, at] for k in range(width)]
        step = cholesky_substitute(columns, scales, right, width, tile)
        for q in range(blocks):
            rows = slice(SUB * q, SUB * q + SUB)
            new_ref[rows, at] = vt_ref[rows, at] + step[q]
        fixed = seen([width * groups + g for g in lanes], 1) + sum_ref[0:1, at] + sums_ref[0:1, at]
        deviance_ref[:, at] = fixed * (2.0 / total_cells)


def kernel_call(body, outs, scratch, flops, limit=8, space=pltpu.VMEM):
    single = pl.BlockSpec(memory_space=pltpu.VMEM)

    def call(*args):
        if space == pltpu.HBM:
            args = [pltpu.with_memory_space_constraint(x, pltpu.HBM) for x in args]
        return pl.pallas_call(
            body,
            out_shape=outs,
            in_specs=[pl.BlockSpec(memory_space=space)] * len(args),
            out_specs=jax.tree.map(lambda _: single, outs),
            scratch_shapes=scratch,
            compiler_params=pltpu.CompilerParams(vmem_limit_bytes=limit * MIB),
            cost_estimate=pl.CostEstimate(flops=flops, bytes_accessed=1 << 20, transcendentals=0),
        )(*args)

    return call


def exchange(x, axis, bit):
    size = lax.axis_size(axis)
    return lax.ppermute(x, axis, [(i, i ^ bit) for i in range(size)])


def sweep(counts, totals, cell_factors, gene_loadings):
    cells, genes = counts.shape
    width = cell_factors.shape[1]
    half = cells // 2
    rows = SUB * len(table_pieces(width))
    shape = functools.partial(jax.ShapeDtypeStruct, dtype=jnp.float32)
    tall = width + SUB
    ut, vt = cell_factors.T, gene_loadings.T
    totals = totals.reshape(1, cells)

    gene_bits = [1 << k for k in range(1, (lax.axis_size("gene") - 1).bit_length())]
    across = [vt]
    for bit in gene_bits:
        across = across + [exchange(x, "gene", bit) for x in across]

    mine, theirs, exact, offset, ut, vt = kernel_call(
        factor_gradient_kernel,
        (
            shape((width, half)),
            shape((width, half)),
            jax.ShapeDtypeStruct((cells, genes), jnp.bfloat16),
            shape((1, cells)),
            shape((width, cells)),
            shape((width, genes)),
        ),
        [pltpu.VMEM((cells, genes), jnp.int32), pltpu.VMEM((1, cells), jnp.int32), pltpu.SemaphoreType.DMA((4,))],
        10**9,
        space=pltpu.HBM,
    )(counts, totals, ut, vt)
    mine = mine + exchange(theirs, "gene", 1)
    for bit in gene_bits[:-1]:
        mine = mine + exchange(mine, "gene", bit)
    other = exchange(mine, "gene", gene_bits[-1])

    moments = ()
    for k, x in enumerate([vt] + across[1:]):
        moments = kernel_call(
            functools.partial(factor_moments_kernel, width, k > 0),
            (shape((rows, half)), shape((rows, half))),
            [pltpu.VMEM((rows, genes), jnp.bfloat16)],
            10**9,
        )(x, offset, ut, *moments)
    moments = (moments[0], exchange(moments[1], "gene", 1))
    block = kernel_call(
        functools.partial(factor_solve_kernel, width, len(moments)), shape((1, tall, half)), [], 10**9
    )(*moments, mine, other, offset, ut)

    cell_bits = [1 << k for k in range((lax.axis_size("cell") - 1).bit_length())]
    gathered = block
    for bit in reversed(cell_bits):
        gathered = jnp.concatenate([gathered, exchange(gathered, "cell", bit)], axis=0)
    partner = exchange(block, "gene", 1)
    opposite = exchange(gathered, "gene", 1)

    factors, linear = kernel_call(
        functools.partial(counts_kernel, width), (shape((width, cells)), shape(((width + 1) * genes // LANES, LANES))), [], 10**9
    )(exact, block, partner, vt)
    for bit in cell_bits[:-1]:
        linear = linear + exchange(linear, "cell", bit)
    linear_other = exchange(linear, "cell", cell_bits[-1])

    per = min(gathered.shape[0], 8)
    tile = 256
    depth = 6 * width + 16

    def moments_of(blocks):
        return kernel_call(
            functools.partial(loading_moments_kernel, width, per, tile),
            (shape((rows + width, genes)), shape((SUB, genes))),
            [
                pltpu.VMEM((rows + width, per * half), jnp.bfloat16),
                pltpu.VMEM((depth, per * half), jnp.bfloat16),
                pltpu.VMEM((depth, genes), jnp.bfloat16),
            ],
            4 * 10**9,
            16,
        )(blocks, vt)

    moments, sums = moments_of(gathered)
    more, more_sums = moments_of(opposite)
    lower, scales = kernel_call(
        functools.partial(loading_factor_kernel, width, 256),
        (shape((rows, genes)), shape((width, genes))),
        [],
        4 * 10**9,
    )(moments, more)
    total_cells = cells * lax.axis_size("cell")
    new_loadings, deviance = kernel_call(
        functools.partial(loading_solve_kernel, width, min(genes, 1024), total_cells),
        (shape((width, genes)), shape((1, genes))),
        [],
        10**9,
    )(lower, scales, moments, more, sums, more_sums, linear, linear_other, vt)
    return (factors.T, new_loadings.T, deviance.reshape(genes))


def solution(mesh):
    return jax.shard_map(
        sweep,
        mesh=mesh,
        in_specs=(P("cell", "gene"), P("cell"), P("cell", None), P("gene", None)),
        out_specs=(P("cell", None), P("gene", None), P("gene")),
        check_vma=False,
    )
```

```python
import functools
import math

import jax
import jax.numpy as jnp
from jax import lax
from jax.experimental import pallas as pl
from jax.experimental.pallas import tpu as pltpu
from jax.sharding import PartitionSpec as P


RIDGE = 1.0
DAMPING = 0.1
SCALE_TOTAL = 5000.0
SUB = 8
LANES = 128
MIB = 1024 * 1024


def table_pieces(width):
    return [(a, q) for a in range(width) for q in range(a // SUB, width // SUB)]


def fill_table(table_ref, x, width):
    pieces = table_pieces(width)
    chunks = [x[SUB * q : SUB * q + SUB] for q in range(width // SUB)]
    for p in range(0, len(pieces), 2):
        pair = [x[a : a + 1] * chunks[q] for a, q in pieces[p : p + 2]]
        table_ref[SUB * p : SUB * (p + 2)] = jnp.concatenate(pair, axis=0).astype(jnp.bfloat16)


def three(x):
    high = x.astype(jnp.bfloat16)
    rest = x - high.astype(jnp.float32)
    mid = rest.astype(jnp.bfloat16)
    low = (rest - mid.astype(jnp.float32)).astype(jnp.bfloat16)
    return high, mid, low


def pad_rows(rows):
    index = lax.broadcasted_iota(jnp.int32, (16, rows[0].shape[1]), 0)
    total = jnp.zeros((16, rows[0].shape[1]), jnp.float32)
    for k, row in enumerate(rows):
        total = jnp.where(index == k, row.astype(jnp.float32), total)
    return total.astype(jnp.bfloat16)


def stack_left(x, offset):
    high, mid, low = three(x)
    return jnp.concatenate([high, mid, high, low, mid, high, pad_rows(list(three(offset)))], axis=0)


def stack_right(y):
    high, mid, low = three(y)
    ones = pad_rows([jnp.ones((1, y.shape[1]), jnp.float32)] * 3)
    return jnp.concatenate([high, high, mid, high, mid, low, ones], axis=0)


def cholesky_columns(get, put, width, lanes):
    blocks = width // SUB
    index = lax.broadcasted_iota(jnp.int32, (SUB, lanes), 0)
    trace = jnp.zeros((SUB, lanes), jnp.float32)
    for k in range(width):
        trace = trace + jnp.where(index == k % SUB, get(k, k // SUB), 0.0)
    shift = RIDGE + DAMPING / width * jnp.sum(trace, axis=0, keepdims=True)
    scales = []
    columns = []
    for k in range(width):
        first = k // SUB
        column = {q: get(k, q) for q in range(first, blocks)}
        column[first] = column[first] + jnp.where(index == k % SUB, shift, 0.0)
        for m in range(k):
            factor = columns[m][first][k % SUB : k % SUB + 1]
            for q in range(first, blocks):
                column[q] = column[q] - columns[m][q] * factor
        scale = lax.rsqrt(column[first][k % SUB : k % SUB + 1])
        column = {q: v * scale for q, v in column.items()}
        for q, v in column.items():
            put(k, q, v)
        columns.append(column)
        scales.append(scale)
    return columns, scales


def cholesky_substitute(columns, scales, right, width, lanes):
    blocks = width // SUB
    index = lax.broadcasted_iota(jnp.int32, (SUB, lanes), 0)
    right = list(right)
    forward = []
    for k in range(width):
        first = k // SUB
        value = right[first][k % SUB : k % SUB + 1] * scales[k]
        forward.append(value)
        for q in range(first, blocks):
            right[q] = right[q] - columns[k][q] * value
    answer = [jnp.zeros((SUB, lanes), jnp.float32)] * blocks
    for k in reversed(range(width)):
        first = k // SUB
        terms = sum(columns[k][q] * answer[q] for q in range(first, blocks))
        value = (forward[k] - jnp.sum(terms, axis=0, keepdims=True)) * scales[k]
        answer[first] = jnp.where(index == k % SUB, value, answer[first])
    return answer


def halves(ref):
    half = ref.shape[1] // 2
    core = lax.rem(lax.axis_index("gene"), 2)
    return [ref[:, pl.ds(pl.multiple_of(index * half, half), half)] for index in (core, 1 - core)]


def factor_gradient_kernel(counts_hbm, totals_hbm, ut_hbm, vt_hbm, mine_ref, theirs_ref, exact_ref, offset_ref, ut_ref, vt_ref, counts_ref, totals_ref, sems):
    copies = [
        pltpu.make_async_copy(source, target, sems.at[k])
        for k, (source, target) in enumerate(
            ((totals_hbm, totals_ref), (ut_hbm, ut_ref), (vt_hbm, vt_ref), (counts_hbm, counts_ref))
        )
    ]
    for copy in copies:
        copy.start()
    for copy in copies[:3]:
        copy.wait()
    half = ut_ref.shape[1] // 2
    core = lax.rem(lax.axis_index("gene"), 2)
    offset_ref[...] = jnp.log(totals_ref[...].astype(jnp.float32)) - math.log(SCALE_TOTAL)
    vt = vt_ref[...]
    right = stack_right(vt)
    low = vt.astype(jnp.bfloat16)
    linear = [
        lax.dot_general(stack_left(ut, offset), right, (((0,), (0,)), ((), ())), preferred_element_type=jnp.float32)
        for ut, offset in zip(halves(ut_ref), halves(offset_ref))
    ]
    copies[3].wait()
    for index, lin, out_ref in ((core, linear[0], mine_ref), (1 - core, linear[1], theirs_ref)):
        part = pl.ds(pl.multiple_of(index * half, half), half)
        counts = counts_ref[part, :].astype(jnp.float32)
        exact_ref[part, :] = counts.astype(jnp.bfloat16)
        residual = (counts - jnp.exp(lin)).astype(jnp.bfloat16)
        out_ref[...] = lax.dot_general(low, residual, (((1,), (1,)), ((), ())), preferred_element_type=jnp.float32)


def factor_moments_kernel(width, add, *refs):
    (vt_ref, offset_ref, ut_ref), before, (mine_ref, theirs_ref, table_ref) = refs[:3], refs[3:-3], refs[-3:]
    half = ut_ref.shape[1] // 2
    vt = vt_ref[...]
    fill_table(table_ref, vt, width)
    left = [stack_left(ut, offset) for ut, offset in zip(halves(ut_ref), halves(offset_ref))]
    linear = lax.dot_general(
        stack_right(vt), jnp.concatenate(left, axis=1), (((0,), (0,)), ((), ())), preferred_element_type=jnp.float32
    )
    weights = jnp.exp(linear).astype(jnp.bfloat16)
    product = jnp.dot(table_ref[...], weights, preferred_element_type=jnp.float32)
    for k, out_ref in enumerate((mine_ref, theirs_ref)):
        total = product[:, k * half : (k + 1) * half]
        if add:
            total = total + before[k][...]
        out_ref[...] = total


def factor_solve_kernel(width, terms, *refs):
    moments, (own_ref, other_ref, offset_ref, ut_ref, new_ref) = refs[:terms], refs[terms:]
    half = own_ref.shape[1]
    place = {piece: SUB * p for p, piece in enumerate(table_pieces(width))}

    def get(a, q):
        at = place[a, q]
        return sum(ref[at : at + SUB, :] for ref in moments)

    ut = halves(ut_ref)[0]
    right = []
    for q in range(width // SUB):
        rows = slice(SUB * q, SUB * q + SUB)
        right.append(own_ref[rows] + other_ref[rows] - RIDGE * ut[rows])
    columns, scales = cholesky_columns(get, lambda a, q, v: None, width, half)
    step = cholesky_substitute(columns, scales, right, width, half)
    new_ref[...] = jnp.zeros_like(new_ref)
    for q in range(width // SUB):
        new_ref[0, SUB * q : SUB * q + SUB, :] = ut[SUB * q : SUB * q + SUB] + step[q]
    new_ref[0, width : width + 1, :] = halves(offset_ref)[0]


def pack(out_ref, square, row, first):
    width = square.shape[0]
    groups = out_ref.shape[0] // (width + 1)
    for j in range(groups):
        cols = slice(first + j * LANES, first + (j + 1) * LANES)
        out_ref[width * j : width * (j + 1), :] = square[:, cols]
        out_ref[width * groups + j : width * groups + j + 1, :] = row[:, cols]


def counts_kernel(width, exact_ref, mine_ref, theirs_ref, vt_ref, factors_ref, own_ref, other_ref, share_ref):
    half = mine_ref.shape[2]
    genes = exact_ref.shape[1]
    core = lax.rem(lax.axis_index("gene"), 2)
    total = jnp.zeros((width, genes), jnp.float32)
    terms = jnp.zeros((1, genes), jnp.float32)
    for index, block_ref in ((core, mine_ref), (1 - core, theirs_ref)):
        part = pl.ds(pl.multiple_of(index * half, half), half)
        block = block_ref[0]
        factors = block[:width]
        factors_ref[:, part] = factors
        exact = exact_ref[part, :]
        high, mid, low = three(factors)
        both = jnp.concatenate([high, mid, low, pad_rows(list(three(block[width : width + 1])))], axis=0)
        product = jnp.dot(both, exact, preferred_element_type=jnp.float32)
        total = total + product[:width]
        full = product[:width] + (product[width : 2 * width] + product[2 * width : 3 * width])
        terms = terms - jnp.sum(full * vt_ref[...], axis=0, keepdims=True)
        terms = terms - jnp.sum(product[3 * width : 3 * width + SUB], axis=0, keepdims=True)
        counts = exact.astype(jnp.float32)
        own_terms = counts * (jnp.log(jnp.maximum(counts, 1.0)) - 1.0)
        terms = terms + jnp.sum(own_terms, axis=0, keepdims=True)
    share = genes // 2
    turn = lax.rem(lax.axis_index("cell"), 2)
    share_ref[...] = vt_ref[:, pl.ds(pl.multiple_of(turn * share, share), share)]
    for k in range(2):

        @pl.when(turn == k)
        def _():
            pack(own_ref, total, terms, k * share)
            pack(other_ref, total, terms, (1 - k) * share)


def loading_moments_kernel(width, per, tile, blocks_ref, vt_ref, out_ref, sum_ref, table_ref, left_ref, right_ref):
    genes = vt_ref.shape[1]
    half = blocks_ref.shape[2]
    groups = blocks_ref.shape[0] // per
    rows = SUB * len(table_pieces(width))
    right_ref[...] = stack_right(vt_ref[...])
    if groups > 1:
        out_ref[...] = jnp.zeros_like(out_ref)
        sum_ref[...] = jnp.zeros_like(sum_ref)

    @pl.loop(0, groups)
    def _(group):
        for b in range(per):
            block = blocks_ref[group * per + b]
            factors = block[:width]
            cols = slice(b * half, (b + 1) * half)
            fill_table(table_ref.at[:, cols], factors, width)
            table_ref[rows : rows + width, cols] = factors.astype(jnp.bfloat16)
            left_ref[:, cols] = stack_left(factors, block[width : width + 1])

        @pl.loop(0, genes // tile)
        def _(j):
            at = pl.ds(pl.multiple_of(j * tile, tile), tile)
            linear = lax.dot_general(
                left_ref[...], right_ref[:, at], (((0,), (0,)), ((), ())), preferred_element_type=jnp.float32
            )
            expected = jnp.exp(linear)
            total = jnp.sum(expected, axis=0, keepdims=True)
            product = jnp.dot(table_ref[...], expected.astype(jnp.bfloat16), preferred_element_type=jnp.float32)
            if groups > 1:
                sum_ref[0:1, at] += total
                out_ref[:, at] += product
            else:
                sum_ref[0:1, at] = total
                out_ref[:, at] = product


def loading_factor_kernel(width, tile, moments_ref, more_ref, lower_ref, scale_ref):
    genes = moments_ref.shape[1]
    place = {piece: SUB * p for p, piece in enumerate(table_pieces(width))}

    @pl.loop(0, genes // tile)
    def _(j):
        at = pl.ds(pl.multiple_of(j * tile, tile), tile)

        def get(a, q):
            rows = slice(place[a, q], place[a, q] + SUB)
            return moments_ref[rows, at] + more_ref[rows, at]

        def put(a, q, value):
            lower_ref[place[a, q] : place[a, q] + SUB, at] = value

        _, scales = cholesky_columns(get, put, width, tile)
        for k in range(width):
            scale_ref[k : k + 1, at] = scales[k]


def loading_solve_kernel(width, tile, total_cells, lower_ref, scale_ref, moments_ref, more_ref, sum_ref, sums_ref, own_ref, other_ref, vt_ref, result_ref):
    genes = vt_ref.shape[1]
    place = {piece: SUB * p for p, piece in enumerate(table_pieces(width))}
    base = SUB * len(place)
    blocks = width // SUB

    groups = genes // LANES

    def seen(first, count):
        parts = [own_ref[f : f + count] + other_ref[f : f + count] for f in first]
        return jnp.concatenate(parts, axis=1)

    for j in range(genes // tile):
        at = slice(j * tile, (j + 1) * tile)
        lanes = range(j * tile // LANES, (j + 1) * tile // LANES)
        right = []
        for q in range(blocks):
            rows = slice(SUB * q, SUB * q + SUB)
            expected = moments_ref[base + SUB * q : base + SUB * q + SUB, at]
            expected = expected + more_ref[base + SUB * q : base + SUB * q + SUB, at]
            counted = seen([width * g + SUB * q for g in lanes], SUB)
            right.append(counted - expected - RIDGE * vt_ref[rows, at])
        columns = [
            {q: lower_ref[place[k, q] : place[k, q] + SUB, at] for q in range(k // SUB, blocks)} for k in range(width)
        ]
        scales = [scale_ref[k : k + 1, at] for k in range(width)]
        step = cholesky_substitute(columns, scales, right, width, tile)
        fixed = seen([width * groups + g for g in lanes], 1) + sum_ref[0:1, at] + sums_ref[0:1, at]
        fixed = fixed * (2.0 / total_cells)
        for g in lanes:
            cols = slice(g * LANES - j * tile, (g + 1) * LANES - j * tile)
            for q in range(blocks):
                rows = slice(SUB * q, SUB * q + SUB)
                here = slice(width * g + SUB * q, width * g + SUB * q + SUB)
                result_ref[here, :] = vt_ref[rows, at][:, cols] + step[q][:, cols]
            result_ref[width * groups + g : width * groups + g + 1, :] = fixed[:, cols]


def assemble_kernel(width, own_ref, other_ref, new_ref, deviance_ref):
    groups = own_ref.shape[0] // (width + 1)
    share = groups * LANES
    turn = lax.rem(lax.axis_index("cell"), 2)
    for first, ref in ((turn, own_ref), (1 - turn, other_ref)):
        for g in range(groups):
            at = pl.ds(pl.multiple_of(first * share + g * LANES, LANES), LANES)
            new_ref[:, at] = ref[width * g : width * (g + 1), :]
            deviance_ref[:, at] = ref[width * groups + g : width * groups + g + 1, :]


def kernel_call(body, outs, scratch, flops, limit=8, space=pltpu.VMEM):
    single = pl.BlockSpec(memory_space=pltpu.VMEM)

    def call(*args):
        if space == pltpu.HBM:
            args = [pltpu.with_memory_space_constraint(x, pltpu.HBM) for x in args]
        return pl.pallas_call(
            body,
            out_shape=outs,
            in_specs=[pl.BlockSpec(memory_space=space)] * len(args),
            out_specs=jax.tree.map(lambda _: single, outs),
            scratch_shapes=scratch,
            compiler_params=pltpu.CompilerParams(vmem_limit_bytes=limit * MIB),
            cost_estimate=pl.CostEstimate(flops=flops, bytes_accessed=1 << 20, transcendentals=0),
        )(*args)

    return call


def exchange(x, axis, bit):
    size = lax.axis_size(axis)
    return lax.ppermute(x, axis, [(i, i ^ bit) for i in range(size)])


def sweep(counts, totals, cell_factors, gene_loadings):
    cells, genes = counts.shape
    width = cell_factors.shape[1]
    half = cells // 2
    rows = SUB * len(table_pieces(width))
    shape = functools.partial(jax.ShapeDtypeStruct, dtype=jnp.float32)
    tall = width + SUB
    ut, vt = cell_factors.T, gene_loadings.T
    totals = totals.reshape(1, cells)

    gene_bits = [1 << k for k in range(1, (lax.axis_size("gene") - 1).bit_length())]
    across = [vt]
    for bit in gene_bits:
        across = across + [exchange(x, "gene", bit) for x in across]

    mine, theirs, exact, offset, ut, vt = kernel_call(
        factor_gradient_kernel,
        (
            shape((width, half)),
            shape((width, half)),
            jax.ShapeDtypeStruct((cells, genes), jnp.bfloat16),
            shape((1, cells)),
            shape((width, cells)),
            shape((width, genes)),
        ),
        [pltpu.VMEM((cells, genes), jnp.int32), pltpu.VMEM((1, cells), jnp.int32), pltpu.SemaphoreType.DMA((4,))],
        10**9,
        space=pltpu.HBM,
    )(counts, totals, ut, vt)
    mine = mine + exchange(theirs, "gene", 1)
    for bit in gene_bits[:-1]:
        mine = mine + exchange(mine, "gene", bit)
    other = exchange(mine, "gene", gene_bits[-1])

    moments = ()
    for k, x in enumerate([vt] + across[1:]):
        moments = kernel_call(
            functools.partial(factor_moments_kernel, width, k > 0),
            (shape((rows, half)), shape((rows, half))),
            [pltpu.VMEM((rows, genes), jnp.bfloat16)],
            10**9,
        )(x, offset, ut, *moments)
    moments = (moments[0], exchange(moments[1], "gene", 1))
    block = kernel_call(
        functools.partial(factor_solve_kernel, width, len(moments)), shape((1, tall, half)), [], 10**9
    )(*moments, mine, other, offset, ut)

    cell_bits = [1 << k for k in range((lax.axis_size("cell") - 1).bit_length())]
    gathered = block
    for bit in reversed(cell_bits):
        arrived = exchange(gathered, "cell", bit)
        gathered = jnp.concatenate([gathered, arrived], axis=0)
    partner = exchange(block, "gene", 1)
    opposite = exchange(gathered, "gene", 1)

    share = genes // 2
    packed = shape(((width + 1) * share // LANES, LANES))
    factors, linear, theirs, vt = kernel_call(
        functools.partial(counts_kernel, width),
        (shape((width, cells)), packed, packed, shape((width, share))),
        [],
        10**9,
    )(exact, block, partner, vt)
    arrived = exchange(theirs, "cell", 1)
    for bit in cell_bits[1:]:
        linear = linear + arrived
        arrived = exchange(linear, "cell", bit)
    per = min(gathered.shape[0], 8)
    tile = 256
    depth = 6 * width + 16

    def moments_of(blocks):
        return kernel_call(
            functools.partial(loading_moments_kernel, width, per, tile),
            (shape((rows + width, share)), shape((SUB, share))),
            [
                pltpu.VMEM((rows + width, per * half), jnp.bfloat16),
                pltpu.VMEM((depth, per * half), jnp.bfloat16),
                pltpu.VMEM((depth, share), jnp.bfloat16),
            ],
            4 * 10**9,
            16,
        )(blocks, vt)

    moments, sums = moments_of(gathered)
    more, more_sums = moments_of(opposite)
    lower, scales = kernel_call(
        functools.partial(loading_factor_kernel, width, 256),
        (shape((rows, share)), shape((width, share))),
        [],
        4 * 10**9,
    )(moments, more)
    total_cells = cells * lax.axis_size("cell")
    result = kernel_call(
        functools.partial(loading_solve_kernel, width, min(share, 512), total_cells), packed, [], 10**9
    )(lower, scales, moments, more, sums, more_sums, linear, arrived, vt)
    new_loadings, deviance = kernel_call(
        functools.partial(assemble_kernel, width), (shape((width, genes)), shape((1, genes))), [], 10**6
    )(result, exchange(result, "cell", 1))
    return (factors.T, new_loadings.T, deviance.reshape(genes))


def solution(mesh):
    return jax.shard_map(
        sweep,
        mesh=mesh,
        in_specs=(P("cell", "gene"), P("cell"), P("cell", None), P("gene", None)),
        out_specs=(P("cell", None), P("gene", None), P("gene")),
        check_vma=False,
    )
```

```python
import functools
import math

import jax
import jax.numpy as jnp
from jax import lax
from jax.experimental import pallas as pl
from jax.experimental.pallas import tpu as pltpu
from jax.sharding import PartitionSpec as P


RIDGE = 1.0
DAMPING = 0.1
SCALE_TOTAL = 5000.0
SUB = 8
LANES = 128
MIB = 1024 * 1024


def table_pieces(width):
    return [(a, q) for a in range(width) for q in range(a // SUB, width // SUB)]


def fill_table(table_ref, x, width):
    pieces = table_pieces(width)
    chunks = [x[SUB * q : SUB * q + SUB] for q in range(width // SUB)]
    for p in range(0, len(pieces), 2):
        pair = [x[a : a + 1] * chunks[q] for a, q in pieces[p : p + 2]]
        table_ref[SUB * p : SUB * (p + 2)] = jnp.concatenate(pair, axis=0).astype(jnp.bfloat16)


def three(x):
    high = x.astype(jnp.bfloat16)
    rest = x - high.astype(jnp.float32)
    mid = rest.astype(jnp.bfloat16)
    low = (rest - mid.astype(jnp.float32)).astype(jnp.bfloat16)
    return high, mid, low


def pad_rows(rows):
    index = lax.broadcasted_iota(jnp.int32, (16, rows[0].shape[1]), 0)
    total = jnp.zeros((16, rows[0].shape[1]), jnp.float32)
    for k, row in enumerate(rows):
        total = jnp.where(index == k, row.astype(jnp.float32), total)
    return total.astype(jnp.bfloat16)


def stack_left(x, offset):
    high, mid, low = three(x)
    return jnp.concatenate([high, mid, high, low, mid, high, pad_rows(list(three(offset)))], axis=0)


def stack_right(y):
    high, mid, low = three(y)
    ones = pad_rows([jnp.ones((1, y.shape[1]), jnp.float32)] * 3)
    return jnp.concatenate([high, high, mid, high, mid, low, ones], axis=0)


def cholesky_columns(get, lower_ref, place, width, lanes):
    blocks = width // SUB
    index = lax.broadcasted_iota(jnp.int32, (SUB, lanes), 0)
    trace = jnp.zeros((SUB, lanes), jnp.float32)
    for k in range(width):
        trace = trace + jnp.where(index == k % SUB, get(k, k // SUB), 0.0)
    shift = RIDGE + DAMPING / width * jnp.sum(trace, axis=0, keepdims=True)
    scales = []
    for k in range(width):
        first = k // SUB
        column = {q: get(k, q) for q in range(first, blocks)}
        column[first] = column[first] + jnp.where(index == k % SUB, shift, 0.0)
        for m in range(k):
            factor = lower_ref[pl.ds(place[m, first] + k % SUB, SUB, stride=0), :]
            for q in range(first, blocks):
                column[q] = column[q] - lower_ref[place[m, q] : place[m, q] + SUB, :] * factor
        scale = lax.rsqrt(column[first][k % SUB : k % SUB + 1])
        for q, v in column.items():
            lower_ref[place[k, q] : place[k, q] + SUB, :] = v * scale
        scales.append(scale)
    return scales


def stored_columns(lower_ref, place, width):
    return [
        {q: lower_ref[place[k, q] : place[k, q] + SUB, :] for q in range(k // SUB, width // SUB)} for k in range(width)
    ]


def cholesky_substitute(columns, scales, right, width, lanes):
    blocks = width // SUB
    index = lax.broadcasted_iota(jnp.int32, (SUB, lanes), 0)
    right = list(right)
    forward = []
    for k in range(width):
        first = k // SUB
        value = right[first][k % SUB : k % SUB + 1] * scales[k]
        forward.append(value)
        for q in range(first, blocks):
            right[q] = right[q] - columns[k][q] * value
    answer = [jnp.zeros((SUB, lanes), jnp.float32)] * blocks
    for k in reversed(range(width)):
        first = k // SUB
        terms = sum(columns[k][q] * answer[q] for q in range(first, blocks))
        value = (forward[k] - jnp.sum(terms, axis=0, keepdims=True)) * scales[k]
        answer[first] = jnp.where(index == k % SUB, value, answer[first])
    return answer


def halves(ref):
    half = ref.shape[1] // 2
    core = lax.rem(lax.axis_index("gene"), 2)
    return [ref[:, pl.ds(pl.multiple_of(index * half, half), half)] for index in (core, 1 - core)]


def factor_gradient_kernel(counts_hbm, totals_hbm, ut_hbm, vt_hbm, mine_ref, theirs_ref, exact_ref, offset_ref, ut_ref, vt_ref, counts_ref, totals_ref, sems):
    copies = [
        pltpu.make_async_copy(source, target, sems.at[k])
        for k, (source, target) in enumerate(
            ((totals_hbm, totals_ref), (ut_hbm, ut_ref), (vt_hbm, vt_ref), (counts_hbm, counts_ref))
        )
    ]
    for copy in copies:
        copy.start()
    for copy in copies[:3]:
        copy.wait()
    half = ut_ref.shape[1] // 2
    core = lax.rem(lax.axis_index("gene"), 2)
    offset_ref[...] = jnp.log(totals_ref[...].astype(jnp.float32)) - math.log(SCALE_TOTAL)
    vt = vt_ref[...]
    right = stack_right(vt)
    low = vt.astype(jnp.bfloat16)
    linear = [
        lax.dot_general(stack_left(ut, offset), right, (((0,), (0,)), ((), ())), preferred_element_type=jnp.float32)
        for ut, offset in zip(halves(ut_ref), halves(offset_ref))
    ]
    copies[3].wait()
    for index, lin, out_ref in ((core, linear[0], mine_ref), (1 - core, linear[1], theirs_ref)):
        part = pl.ds(pl.multiple_of(index * half, half), half)
        counts = counts_ref[part, :].astype(jnp.float32)
        exact_ref[part, :] = counts.astype(jnp.bfloat16)
        residual = (counts - jnp.exp(lin)).astype(jnp.bfloat16)
        out_ref[...] = lax.dot_general(low, residual, (((1,), (1,)), ((), ())), preferred_element_type=jnp.float32)


def factor_moments_kernel(width, step, add, *refs):
    (vt_ref, offset_ref, ut_ref), before, (mine_ref, theirs_ref, table_ref) = refs[:3], refs[3:-3], refs[-3:]
    half = ut_ref.shape[1] // 2
    genes = vt_ref.shape[1]
    left = [stack_left(ut, offset) for ut, offset in zip(halves(ut_ref), halves(offset_ref))]
    left = jnp.concatenate(left, axis=1)
    chunks = [slice(first, first + step) for first in range(0, genes, step)]

    def weigh(cols):
        right = stack_right(vt_ref[:, cols])
        linear = lax.dot_general(right, left, (((0,), (0,)), ((), ())), preferred_element_type=jnp.float32)
        return jnp.exp(linear).astype(jnp.bfloat16)

    weights = []
    for cols in chunks:
        weights.append(weigh(cols))
        fill_table(table_ref.at[:, cols], vt_ref[:, cols], width)
    product = sum(
        jnp.dot(table_ref[:, cols], part, preferred_element_type=jnp.float32) for cols, part in zip(chunks, weights)
    )
    for k, out_ref in enumerate((mine_ref, theirs_ref)):
        total = product[:, k * half : (k + 1) * half]
        if add:
            total = total + before[k][...]
        out_ref[...] = total


def factor_solve_kernel(width, terms, *refs):
    moments, (own_ref, other_ref, offset_ref, ut_ref, new_ref, lower_ref) = refs[:terms], refs[terms:]
    half = own_ref.shape[1]
    place = {piece: SUB * p for p, piece in enumerate(table_pieces(width))}

    def get(a, q):
        at = place[a, q]
        return sum(ref[at : at + SUB, :] for ref in moments)

    ut = halves(ut_ref)[0]
    right = []
    for q in range(width // SUB):
        rows = slice(SUB * q, SUB * q + SUB)
        right.append(own_ref[rows] + other_ref[rows] - RIDGE * ut[rows])
    scales = cholesky_columns(get, lower_ref, place, width, half)
    columns = stored_columns(lower_ref, place, width)
    step = cholesky_substitute(columns, scales, right, width, half)
    new_ref[...] = jnp.zeros_like(new_ref)
    for q in range(width // SUB):
        new_ref[0, SUB * q : SUB * q + SUB, :] = ut[SUB * q : SUB * q + SUB] + step[q]
    new_ref[0, width : width + 1, :] = halves(offset_ref)[0]


def pack(out_ref, square, row, first):
    width = square.shape[0]
    groups = out_ref.shape[0] // (width + 1)
    for j in range(groups):
        cols = slice(first + j * LANES, first + (j + 1) * LANES)
        out_ref[width * j : width * (j + 1), :] = square[:, cols]
        out_ref[width * groups + j : width * groups + j + 1, :] = row[:, cols]


def counts_kernel(width, exact_ref, mine_ref, theirs_ref, vt_ref, factors_ref, own_ref, other_ref, share_ref):
    half = mine_ref.shape[2]
    genes = exact_ref.shape[1]
    core = lax.rem(lax.axis_index("gene"), 2)
    total = jnp.zeros((width, genes), jnp.float32)
    terms = jnp.zeros((1, genes), jnp.float32)
    for index, block_ref in ((core, mine_ref), (1 - core, theirs_ref)):
        part = pl.ds(pl.multiple_of(index * half, half), half)
        block = block_ref[0]
        factors = block[:width]
        factors_ref[:, part] = factors
        exact = exact_ref[part, :]
        high, mid, low = three(factors)
        both = jnp.concatenate([high, mid, low, pad_rows(list(three(block[width : width + 1])))], axis=0)
        product = jnp.dot(both, exact, preferred_element_type=jnp.float32)
        total = total + product[:width]
        full = product[:width] + (product[width : 2 * width] + product[2 * width : 3 * width])
        terms = terms - jnp.sum(full * vt_ref[...], axis=0, keepdims=True)
        terms = terms - jnp.sum(product[3 * width : 3 * width + SUB], axis=0, keepdims=True)
        counts = exact.astype(jnp.float32)
        own_terms = counts * (jnp.log(jnp.maximum(counts, 1.0)) - 1.0)
        terms = terms + jnp.sum(own_terms, axis=0, keepdims=True)
    share = genes // 2
    turn = lax.rem(lax.axis_index("cell"), 2)
    share_ref[...] = vt_ref[:, pl.ds(pl.multiple_of(turn * share, share), share)]
    for k in range(2):

        @pl.when(turn == k)
        def _():
            pack(own_ref, total, terms, k * share)
            pack(other_ref, total, terms, (1 - k) * share)


def loading_moments_kernel(width, per, tile, blocks_ref, vt_ref, out_ref, sum_ref, table_ref, left_ref, right_ref):
    genes = vt_ref.shape[1]
    half = blocks_ref.shape[2]
    groups = blocks_ref.shape[0] // per
    rows = SUB * len(table_pieces(width))
    right_ref[...] = stack_right(vt_ref[...])

    def prepare(group):
        for b in range(per):
            block = blocks_ref[group * per + b]
            factors = block[:width]
            cols = slice(b * half, (b + 1) * half)
            left_ref[:, cols] = stack_left(factors, block[width : width + 1])
            fill_table(table_ref.at[:, cols], factors, width)
            table_ref[rows : rows + width, cols] = factors.astype(jnp.bfloat16)

    def expect(at):
        linear = lax.dot_general(
            left_ref[...], right_ref[:, at], (((0,), (0,)), ((), ())), preferred_element_type=jnp.float32
        )
        expected = jnp.exp(linear)
        return jnp.sum(expected, axis=0, keepdims=True), expected.astype(jnp.bfloat16)

    def contract(weights):
        return jnp.dot(table_ref[...], weights, preferred_element_type=jnp.float32)

    if groups == 1:
        prepare(0)
        tiles = [slice(j * tile, (j + 1) * tile) for j in range(genes // tile)]
        found = [expect(at) for at in tiles]
        for at, (total, weights) in zip(tiles, found):
            sum_ref[0:1, at] = total
            out_ref[:, at] = contract(weights)
        return
    out_ref[...] = jnp.zeros_like(out_ref)
    sum_ref[...] = jnp.zeros_like(sum_ref)

    @pl.loop(0, groups)
    def _(group):
        prepare(group)

        @pl.loop(0, genes // tile)
        def _(j):
            at = pl.ds(pl.multiple_of(j * tile, tile), tile)
            total, weights = expect(at)
            sum_ref[0:1, at] += total
            out_ref[:, at] += contract(weights)


def loading_factor_kernel(width, tile, moments_ref, more_ref, lower_ref, scale_ref):
    genes = moments_ref.shape[1]
    place = {piece: SUB * p for p, piece in enumerate(table_pieces(width))}

    for j in range(genes // tile):
        at = slice(j * tile, (j + 1) * tile)

        def get(a, q, at=at):
            rows = slice(place[a, q], place[a, q] + SUB)
            return moments_ref[rows, at] + more_ref[rows, at]

        scales = cholesky_columns(get, lower_ref.at[j], place, width, tile)
        for k in range(width):
            scale_ref[k : k + 1, at] = scales[k]


def loading_solve_kernel(width, tile, total_cells, lower_ref, scale_ref, moments_ref, more_ref, sum_ref, sums_ref, own_ref, other_ref, vt_ref, result_ref):
    genes = vt_ref.shape[1]
    place = {piece: SUB * p for p, piece in enumerate(table_pieces(width))}
    base = SUB * len(place)
    blocks = width // SUB

    groups = genes // LANES

    def seen(first, count):
        parts = [own_ref[f : f + count] + other_ref[f : f + count] for f in first]
        return jnp.concatenate(parts, axis=1)

    for j in range(genes // tile):
        at = slice(j * tile, (j + 1) * tile)
        lanes = range(j * tile // LANES, (j + 1) * tile // LANES)
        right = []
        for q in range(blocks):
            rows = slice(SUB * q, SUB * q + SUB)
            expected = moments_ref[base + SUB * q : base + SUB * q + SUB, at]
            expected = expected + more_ref[base + SUB * q : base + SUB * q + SUB, at]
            counted = seen([width * g + SUB * q for g in lanes], SUB)
            right.append(counted - expected - RIDGE * vt_ref[rows, at])
        columns = stored_columns(lower_ref.at[j], place, width)
        scales = [scale_ref[k : k + 1, at] for k in range(width)]
        step = cholesky_substitute(columns, scales, right, width, tile)
        fixed = seen([width * groups + g for g in lanes], 1) + sum_ref[0:1, at] + sums_ref[0:1, at]
        fixed = fixed * (2.0 / total_cells)
        for g in lanes:
            cols = slice(g * LANES - j * tile, (g + 1) * LANES - j * tile)
            for q in range(blocks):
                rows = slice(SUB * q, SUB * q + SUB)
                here = slice(width * g + SUB * q, width * g + SUB * q + SUB)
                result_ref[here, :] = vt_ref[rows, at][:, cols] + step[q][:, cols]
            result_ref[width * groups + g : width * groups + g + 1, :] = fixed[:, cols]


def assemble_kernel(width, own_ref, other_ref, new_ref, deviance_ref):
    groups = own_ref.shape[0] // (width + 1)
    share = groups * LANES
    turn = lax.rem(lax.axis_index("cell"), 2)
    for first, ref in ((turn, own_ref), (1 - turn, other_ref)):
        for g in range(groups):
            at = pl.ds(pl.multiple_of(first * share + g * LANES, LANES), LANES)
            new_ref[:, at] = ref[width * g : width * (g + 1), :]
            deviance_ref[:, at] = ref[width * groups + g : width * groups + g + 1, :]


def kernel_call(body, outs, scratch, flops, limit=8, space=pltpu.VMEM):
    single = pl.BlockSpec(memory_space=pltpu.VMEM)

    def call(*args):
        if space == pltpu.HBM:
            args = [pltpu.with_memory_space_constraint(x, pltpu.HBM) for x in args]
        return pl.pallas_call(
            body,
            out_shape=outs,
            in_specs=[pl.BlockSpec(memory_space=space)] * len(args),
            out_specs=jax.tree.map(lambda _: single, outs),
            scratch_shapes=scratch,
            compiler_params=pltpu.CompilerParams(vmem_limit_bytes=limit * MIB),
            cost_estimate=pl.CostEstimate(flops=flops, bytes_accessed=1 << 20, transcendentals=0),
        )(*args)

    return call


def exchange(x, axis, bit):
    size = lax.axis_size(axis)
    return lax.ppermute(x, axis, [(i, i ^ bit) for i in range(size)])


def sweep(counts, totals, cell_factors, gene_loadings):
    cells, genes = counts.shape
    width = cell_factors.shape[1]
    half = cells // 2
    rows = SUB * len(table_pieces(width))
    shape = functools.partial(jax.ShapeDtypeStruct, dtype=jnp.float32)
    tall = width + SUB
    ut, vt = cell_factors.T, gene_loadings.T
    totals = totals.reshape(1, cells)

    gene_bits = [1 << k for k in range(1, (lax.axis_size("gene") - 1).bit_length())]
    across = [vt]
    for bit in gene_bits:
        across = across + [exchange(x, "gene", bit) for x in across]

    mine, theirs, exact, offset, ut, vt = kernel_call(
        factor_gradient_kernel,
        (
            shape((width, half)),
            shape((width, half)),
            jax.ShapeDtypeStruct((cells, genes), jnp.bfloat16),
            shape((1, cells)),
            shape((width, cells)),
            shape((width, genes)),
        ),
        [pltpu.VMEM((cells, genes), jnp.int32), pltpu.VMEM((1, cells), jnp.int32), pltpu.SemaphoreType.DMA((4,))],
        10**9,
        space=pltpu.HBM,
    )(counts, totals, ut, vt)
    mine = mine + exchange(theirs, "gene", 1)
    for bit in gene_bits[:-1]:
        mine = mine + exchange(mine, "gene", bit)
    other = exchange(mine, "gene", gene_bits[-1])

    moments = ()
    for k, x in enumerate([vt] + across[1:]):
        moments = kernel_call(
            functools.partial(factor_moments_kernel, width, genes // 2, k > 0),
            (shape((rows, half)), shape((rows, half))),
            [pltpu.VMEM((rows, genes), jnp.bfloat16)],
            10**9,
        )(x, offset, ut, *moments)
    moments = (moments[0], exchange(moments[1], "gene", 1))
    block = kernel_call(
        functools.partial(factor_solve_kernel, width, len(moments)),
        shape((1, tall, half)),
        [pltpu.VMEM((rows, half), jnp.float32)],
        10**9,
    )(*moments, mine, other, offset, ut)

    cell_bits = [1 << k for k in range((lax.axis_size("cell") - 1).bit_length())]
    gathered = block
    for bit in reversed(cell_bits):
        arrived = exchange(gathered, "cell", bit)
        gathered = jnp.concatenate([gathered, arrived], axis=0)
    partner = exchange(block, "gene", 1)
    opposite = exchange(gathered, "gene", 1)

    share = genes // 2
    packed = shape(((width + 1) * share // LANES, LANES))
    factors, linear, theirs, vt = kernel_call(
        functools.partial(counts_kernel, width),
        (shape((width, cells)), packed, packed, shape((width, share))),
        [],
        10**9,
    )(exact, block, partner, vt)
    arrived = exchange(theirs, "cell", 1)
    for bit in cell_bits[1:]:
        linear = linear + arrived
        arrived = exchange(linear, "cell", bit)
    per = min(gathered.shape[0], 8)
    tile = 256
    depth = 6 * width + 16

    def moments_of(blocks):
        return kernel_call(
            functools.partial(loading_moments_kernel, width, per, tile),
            (shape((rows + width, share)), shape((SUB, share))),
            [
                pltpu.VMEM((rows + width, per * half), jnp.bfloat16),
                pltpu.VMEM((depth, per * half), jnp.bfloat16),
                pltpu.VMEM((depth, share), jnp.bfloat16),
            ],
            4 * 10**9,
            16,
        )(blocks, vt)

    moments, sums = moments_of(gathered)
    more, more_sums = moments_of(opposite)
    lanes = min(share, 512)
    lower, scales = kernel_call(
        functools.partial(loading_factor_kernel, width, lanes),
        (shape((share // lanes, rows, lanes)), shape((width, share))),
        [],
        4 * 10**9,
    )(moments, more)
    total_cells = cells * lax.axis_size("cell")
    result = kernel_call(
        functools.partial(loading_solve_kernel, width, lanes, total_cells), packed, [], 10**9
    )(lower, scales, moments, more, sums, more_sums, linear, arrived, vt)
    new_loadings, deviance = kernel_call(
        functools.partial(assemble_kernel, width), (shape((width, genes)), shape((1, genes))), [], 10**6
    )(result, exchange(result, "cell", 1))
    return (factors.T, new_loadings.T, deviance.reshape(genes))


def solution(mesh):
    return jax.shard_map(
        sweep,
        mesh=mesh,
        in_specs=(P("cell", "gene"), P("cell"), P("cell", None), P("gene", None)),
        out_specs=(P("cell", None), P("gene", None), P("gene")),
        check_vma=False,
    )
```
